32 devices in a mesh: ctx: 16 (over z, y, core), head: 2 (over x).
Axes of the slice: x: 2, y: 2, z: 4, core: 2. Of those that a mesh axis runs over, the one named last changes fastest.
Arguments:
- queries: bfloat16 [8192, 16, 128], P('ctx', 'head'), may hold values from -130 to 130, as said below
- values: bfloat16 [8192, 16, 128], P('ctx', 'head'), may hold values from -6 to 6
- codes: int32 [8192, 16], P('ctx', 'head'), may hold values from 0 to 511
- codebook: bfloat16 [16, 512, 128], P('head'), may hold values from -8 to 8, as said below
- out_weight: bfloat16 [2048, 2048], P('head'), may hold values from -0.1875 to 0.1875
Outputs:
- mixed: bfloat16 [8192, 2048], P('ctx', 'head')
The draws below stay inside these ranges and needn't reach their ends.
Inputs may be any that keep to these rules, and one draw needn't show every extreme that they name: `queries`: every entry has magnitude at most 130. `codebook`: every entry has magnitude at most 8.
All inputs are finite; a program needn't handle non-finite values.
Results may differ from the reference program's by a relative error of at most 0.0066.
Values may be sent and summed in bfloat16 or wider, within the bound.
No kernel may reach another device: no remote copies, remote signals or barrier semaphores. Data moves between devices by JAX's collectives and lax.ppermute only.
A program may use at most 128 MiB of HBM per device.

```python
import jax
import jax.numpy as jnp
from jax import lax

D = 2048
HEADS = 16
DH = 128
CODES = 512
BLOCK = 512
TOKENS = 8192


def shared_codebook(key):
    base = jax.random.truncated_normal(jax.random.fold_in(key, 11), -6.0, 6.0, (HEADS, CODES, DH), jnp.float32)
    return base


def draw_codebook(key, part):
    return shared_codebook(key).astype(jnp.bfloat16)


def draw_queries(key, part):
    drawn = jax.random.truncated_normal(jax.random.fold_in(key, 21), -6.0, 6.0, (TOKENS, HEADS, DH), jnp.float32)
    return drawn.astype(jnp.bfloat16)


def set_ends(values, rng, smallest, high):
    extent = values.shape
    spot = [jax.random.randint(jax.random.fold_in(rng, axis), (), 0, extent[axis]) for axis in range(len(extent))]
    values = values.at[tuple(spot)].set(smallest)
    longest = extent.index(max(extent))
    spot[longest] = (spot[longest] + 1) % extent[longest]
    return values.at[tuple(spot)].set(high)


def with_spikes(result, rng, source, target, parts, factor):
    owner, partner = [(jnp.arange(result.shape[dim]) // (result.shape[dim] // parts)).reshape([-1 if axis == dim else 1 for axis in range(result.ndim)]) for dim in (source, target)]
    chosen = jax.random.permutation(rng, parts)[partner]
    strong = (owner == chosen) | (owner == (partner + parts // 2) % parts)
    return jnp.where(strong, factor * result, result)


def level_of(own_key, extent, split, smallest, high):
    level, own = 1.0, jax.random.fold_in(own_key, 6)
    for axis_at, blocks in split:
        heights = jnp.exp(jax.random.uniform(jax.random.fold_in(own, axis_at), (blocks,), jnp.float32, smallest / len(split), high / len(split)))
        level = level * jnp.repeat(heights, extent[axis_at] // blocks).reshape([-1 if axis == axis_at else 1 for axis in range(len(extent))])
    return level


def gaussian(rng, dims, scale, most, shards=(), dtype=jnp.bfloat16):
    result = scale * jax.random.normal(rng, dims, jnp.float32)
    if shards:
        result = result * level_of(rng, dims, shards, -0.22, 0.18)
    return jnp.clip(result, -most, most).astype(dtype)


def gaussian_with(key, shape, deviation, reach, pieces, heavy, kind=jnp.bfloat16):
    values = deviation * jax.random.normal(key, shape, jnp.float32)
    if pieces:
        values = values * level_of(key, shape, pieces, -0.22, 0.18)
    return jnp.clip(with_spikes(values, jax.random.fold_in(key, 3), *heavy), -reach, reach).astype(kind)


def setup_inputs(seed: int = 0) -> dict:
    key_list = jax.random.split(jax.random.key(seed), 6)
    queries = draw_queries(jax.random.fold_in(key_list[5], 71), 0)
    values = gaussian(key_list[1], (TOKENS, HEADS, DH), 1.0, 6.0, ((0, 16), (1, 2)))
    codes = set_ends(jax.random.randint(key_list[2], (TOKENS, HEADS), 0, CODES), jax.random.fold_in(key_list[2], 1), 0, CODES - 1).astype(jnp.int32)
    codebook = draw_codebook(jax.random.fold_in(key_list[5], 71), 0)
    out_weight = gaussian_with(key_list[4], (HEADS * DH, D), (HEADS * DH) ** -0.5, 0.1875, ((0, 2),), (0, 1, 2, 2.0))
    return dict(queries=queries, values=values, codes=codes, codebook=codebook, out_weight=out_weight)


def attend(query, cur_keys, cur_values, prev_keys, prev_values, live, book, cache_sum, cache_count):
    scale = query.shape[-1] ** -0.5
    code_scores = jnp.dot(query, book.T, preferred_element_type=jnp.float32) * scale
    cur_scores = jnp.dot(query, cur_keys.T, preferred_element_type=jnp.float32) * scale
    prev_scores = jnp.dot(query, prev_keys.T, preferred_element_type=jnp.float32) * scale
    rows = lax.broadcasted_iota(jnp.int32, cur_scores.shape, 0)
    cols = lax.broadcasted_iota(jnp.int32, cur_scores.shape, 1)
    causal = rows >= cols
    present = (cache_count > 0.0)[None, :]
    top = jnp.max(jnp.where(causal, cur_scores, -jnp.inf), axis=1)
    top = jnp.maximum(top, jnp.max(jnp.where(live, prev_scores, -jnp.inf), axis=1))
    top = jnp.maximum(top, jnp.max(jnp.where(present, code_scores, -jnp.inf), axis=1))
    top = top[:, None]
    cur_weight = jnp.where(causal, jnp.exp(cur_scores - top), 0.0)
    prev_weight = jnp.where(live, jnp.exp(prev_scores - top), 0.0)
    code_weight = jnp.where(present, jnp.exp(code_scores - top), 0.0)
    denom = jnp.sum(cur_weight, axis=1) + jnp.sum(prev_weight, axis=1) + jnp.sum(code_weight * cache_count[None, :], axis=1)
    numer = jnp.dot(cur_weight.astype(jnp.bfloat16), cur_values, preferred_element_type=jnp.float32)
    numer = numer + jnp.dot(prev_weight.astype(jnp.bfloat16), prev_values, preferred_element_type=jnp.float32)
    numer = numer + jnp.dot(code_weight, cache_sum, precision=lax.Precision.HIGHEST)
    return (numer / denom[:, None]).astype(jnp.bfloat16)


def reference(queries, values, codes, codebook, out_weight):
    heads = codebook.shape[0]
    width = codebook.shape[2]
    ncodes = codebook.shape[1]
    nblocks = TOKENS // BLOCK
    keys = jax.vmap(lambda book, index: book[index], in_axes=(0, 1), out_axes=1)(codebook, codes)
    query_blocks = queries.reshape(nblocks, BLOCK, heads, width)
    key_blocks = keys.reshape(nblocks, BLOCK, heads, width)
    value_blocks = values.reshape(nblocks, BLOCK, heads, width)
    code_blocks = codes.reshape(nblocks, BLOCK, heads)
    table = lax.broadcasted_iota(jnp.int32, (1, 1, ncodes), 2)

    def step(carry, block):
        cache_sum, cache_count, pend_sum, pend_count, prev_keys, prev_values, live = carry
        query, key, value, index = block
        attended = jax.vmap(attend, in_axes=(1, 1, 1, 1, 1, None, 0, 0, 0), out_axes=1)(
            query, key, value, prev_keys, prev_values, live, codebook, cache_sum, cache_count)
        onehot = (index[:, :, None] == table).astype(jnp.float32)
        sums = jnp.einsum("ths,thd->hsd", onehot, value.astype(jnp.float32), precision=lax.Precision.HIGHEST)
        counts = jnp.sum(onehot, axis=0)
        carry = (cache_sum + pend_sum, cache_count + pend_count, sums, counts, key, value, jnp.array(True))
        return carry, attended

    zero_sum = jnp.zeros((heads, ncodes, width), jnp.float32)
    zero_count = jnp.zeros((heads, ncodes), jnp.float32)
    zero_block = jnp.zeros((BLOCK, heads, width), jnp.bfloat16)
    start = (zero_sum, zero_count, zero_sum, zero_count, zero_block, zero_block, jnp.array(False))
    final, outputs = lax.scan(step, start, (query_blocks, key_blocks, value_blocks, code_blocks))
    attended = outputs.reshape(TOKENS, heads * width)
    return jnp.dot(attended, out_weight, preferred_element_type=jnp.float32).astype(jnp.bfloat16)
```

```python
import functools
import math

import jax
import jax.numpy as jnp
from jax import lax
from jax.experimental import pallas as pl
from jax.experimental.pallas import tpu as pltpu
from jax.sharding import PartitionSpec as P

BLOCK = 512
LANES = 128
GROUPS = 4
NEVER = -1e30
F32 = jnp.float32
BF16 = jnp.bfloat16


def dot(a, b, contract=((1,), (0,))):
    return lax.dot_general(a, b, (contract, ((), ())), preferred_element_type=F32)


class Layout:
    def __init__(self, devices, heads, ncodes):
        self.groups = math.gcd(GROUPS, heads)
        self.heads = heads // self.groups
        self.each = ncodes // LANES
        self.units = self.heads * self.each
        self.per = self.units // 4
        self.shift = int(math.log2(256 // devices + 1))
        self.digits = 1
        while (1 << (self.shift * self.digits)) <= BLOCK:
            self.digits += 1
        self.sums = self.per * LANES
        self.tail = -(-self.digits * self.per // 16) * 16
        self.rows = self.sums + self.tail
        assert ncodes % LANES == 0 and self.units % 4 == 0 and devices % 4 == 0


def sums_kernel(lay, pos_ref, codes_ref, values_ref, *refs):
    outs, buf = (refs[:-1], refs[-1])
    core, row = (pos_ref[0], pos_ref[1])
    heads, tokens = codes_ref.shape
    ncodes = lay.each * LANES
    by_head = jnp.swapaxes(values_ref[...], 0, 1)
    table = lax.broadcasted_iota(jnp.int32, (ncodes, tokens), 0)
    line = lax.broadcasted_iota(jnp.int32, (lay.tail, LANES), 0)
    ones = jnp.ones((8, tokens), BF16)
    mask = (1 << lay.shift) - 1
    for g in range(lay.groups):
        tails = [jnp.zeros((lay.tail, LANES), F32) for _ in range(4)]
        for k in range(lay.heads):
            h = g * lay.heads + k
            onehot = (table == codes_ref[h : h + 1, :]).astype(BF16)
            sums = dot(onehot, by_head[h]).astype(BF16)
            count = dot(ones, onehot, ((1,), (1,)))[0:1].astype(jnp.int32)
            for j in range(lay.each):
                piece, at = divmod(k * lay.each + j, lay.per)
                a, b = (piece // 2 ^ core, piece % 2 ^ row)
                buf[a, b, at * LANES : (at + 1) * LANES, :] = sums[j * LANES : (j + 1) * LANES]
                part = count[:, j * LANES : (j + 1) * LANES]
                for d in range(lay.digits):
                    digit = ((part >> (lay.shift * d)) & mask).astype(F32)
                    tails[piece] = jnp.where(line == d * lay.per + at, digit, tails[piece])
        for piece in range(4):
            buf[piece // 2 ^ core, piece % 2 ^ row, lay.sums :, :] = tails[piece].astype(BF16)
        outs[2 * g][...] = buf[0]
        outs[2 * g + 1][...] = buf[1]


def block_sums(lay, pos, codes, values):
    tokens, heads, width = values.shape
    piece = jax.ShapeDtypeStruct((2, lay.rows, LANES), BF16)
    vmem = pl.BlockSpec(memory_space=pltpu.VMEM)
    outs = pl.pallas_call(
        functools.partial(sums_kernel, lay),
        out_shape=[piece] * (2 * lay.groups),
        in_specs=[pl.BlockSpec(memory_space=pltpu.SMEM), vmem, vmem],
        out_specs=[vmem] * (2 * lay.groups),
        scratch_shapes=[pltpu.VMEM((2, 2, lay.rows, LANES), BF16)],
        cost_estimate=pl.CostEstimate(
            flops=2 * heads * tokens * lay.each * LANES * width * 2, bytes_accessed=4 * tokens * heads * width, transcendentals=0
        ),
        name="block_sums",
    )(pos, codes, values)
    return [(outs[2 * g], outs[2 * g + 1]) for g in range(lay.groups)]


def window_kernel(factor, codes_ref, queries_ref, values_ref, book_ref, qt_ref, num_ref, ml_ref, vt_ref):
    heads, tokens = codes_ref.shape
    ncodes = book_ref.shape[1]
    tile = tokens // 2
    qt_ref[...] = jnp.swapaxes(queries_ref[...], 0, 1)
    vt_ref[...] = jnp.swapaxes(values_ref[...], 0, 1)
    table = lax.broadcasted_iota(jnp.int32, (ncodes, tokens), 0)
    lane = lax.broadcasted_iota(jnp.int32, (tile, LANES), 1)
    causal = lax.broadcasted_iota(jnp.int32, (tile, tile), 0) >= lax.broadcasted_iota(jnp.int32, (tile, tile), 1)

    def one(h, carry):
        onehot = (table == codes_ref[pl.ds(h, 1), :]).astype(BF16)
        keys = dot(book_ref[h], onehot, ((0,), (0,))).astype(BF16)
        value = vt_ref[h]
        for r in range(2):
            rows = slice(r * tile, (r + 1) * tile)
            query = qt_ref[h, rows, :]
            score = jnp.where(causal, dot(query, keys[:, rows]), NEVER)
            top = jnp.max(score, axis=1, keepdims=True)
            if r:
                early = dot(query, keys[:, :tile])
                top = jnp.maximum(top, jnp.max(early, axis=1, keepdims=True))
            weight = jnp.exp2((score - top) * factor)
            den = jnp.sum(weight, axis=1, keepdims=True)
            num = dot(weight.astype(BF16), value[rows])
            if r:
                weight = jnp.exp2((early - top) * factor)
                den += jnp.sum(weight, axis=1, keepdims=True)
                num += dot(weight.astype(BF16), value[:tile])
            num_ref[h, rows, :] = num
            ml_ref[h, rows, :] = jnp.where(lane < LANES // 2, top, den)
        return carry

    lax.fori_loop(0, heads, one, 0)


def window(codes, queries, values, book):
    tokens, heads, width = queries.shape
    vmem = pl.BlockSpec(memory_space=pltpu.VMEM)
    factor = width ** (-0.5) * math.log2(math.e)
    flops = 2 * heads * tokens * tokens * width * 3
    return pl.pallas_call(
        functools.partial(window_kernel, factor),
        out_shape=[
            jax.ShapeDtypeStruct((heads, tokens, width), BF16),
            jax.ShapeDtypeStruct((heads, tokens, width), F32),
            jax.ShapeDtypeStruct((heads, tokens, LANES), F32),
        ],
        in_specs=[vmem] * 4,
        out_specs=[vmem] * 3,
        scratch_shapes=[pltpu.VMEM((heads, tokens, width), BF16)],
        cost_estimate=pl.CostEstimate(flops=flops * 4, bytes_accessed=9 * tokens * heads * width, transcendentals=0),
        name="window",
    )(codes, queries, values, book)


def codes_kernel(lay, factor, pos_ref, qt_ref, book_ref, num_ref, ml_ref, mine_ref, theirs_ref, out_ref):
    core, row = (pos_ref[0], pos_ref[1])
    width = qt_ref.shape[2]

    def piece(p, rows):
        b = p % 2 ^ row
        return jnp.where(p // 2 == core, mine_ref[b, rows, :].astype(F32), theirs_ref[b, rows, :].astype(F32))

    tails = [piece(p, slice(lay.sums, lay.rows)) for p in range(4)]
    for k in range(lay.heads):
        sums, counts = ([], [])
        for j in range(lay.each):
            p, at = divmod(k * lay.each + j, lay.per)
            sums.append(piece(p, slice(at * LANES, (at + 1) * LANES)).astype(BF16))
            count = 0.0
            for d in range(lay.digits):
                line = d * lay.per + at
                count = count + tails[p][line : line + 1] * float(1 << (lay.shift * d))
            counts.append(count)
        cache = jnp.concatenate(sums, axis=0)
        count = jnp.concatenate(counts, axis=1)
        score = dot(qt_ref[k], book_ref[k], ((1,), (1,)))
        score = score + jnp.where(count > 0.5, 0.0, NEVER)
        early = ml_ref[k, :, 0:1]
        top = jnp.maximum(early, jnp.max(score, axis=1, keepdims=True))
        weight = jnp.exp2((score - top) * factor)
        keep = jnp.exp2((early - top) * factor)
        den = keep * ml_ref[k, :, LANES // 2 : LANES // 2 + 1] + jnp.sum(weight * count, axis=1, keepdims=True)
        num = keep * num_ref[k] + dot(weight.astype(BF16), cache)
        out_ref[:, k * width : (k + 1) * width] = (num / den).astype(BF16)


def attend(lay, g, pos, qt, book, num, ml, mine, theirs):
    heads, tokens, width = qt.shape
    ncodes = book.shape[1]
    vmem = pl.BlockSpec(memory_space=pltpu.VMEM)
    factor = width ** (-0.5) * math.log2(math.e)
    part = lambda n: pl.BlockSpec((lay.heads, n, width), lambda i: (g, 0, 0))
    whole = lambda x: pl.BlockSpec(x.shape, lambda i: (0,) * x.ndim)
    out = jax.ShapeDtypeStruct((tokens, lay.heads * width), BF16)
    return pl.pallas_call(
        functools.partial(codes_kernel, lay, factor),
        out_shape=out,
        grid=(1,),
        in_specs=[pl.BlockSpec(memory_space=pltpu.SMEM), part(tokens), part(ncodes), part(tokens), part(tokens), whole(mine), whole(theirs)],
        out_specs=whole(out),
        cost_estimate=pl.CostEstimate(
            flops=2 * lay.heads * tokens * ncodes * width * 8, bytes_accessed=14 * tokens * lay.heads * width, transcendentals=0
        ),
        name="attend",
    )(pos, qt, book, num, ml, mine, theirs)


def swap(x, axis, k):
    return lax.ppermute(x, axis, [(i, i ^ k) for i in range(lax.axis_size(axis))])


def ahead(x, axis, k):
    return lax.ppermute(x, axis, [(i, i + k) for i in range(lax.axis_size(axis) - k)])


def add(a, b):
    return (a.astype(F32) + b.astype(F32)).astype(BF16)


def earlier_totals(x, axis, stride):
    count = lax.axis_size(axis) // stride
    if count <= 4:
        parts = [ahead(x, axis, stride * d) for d in range(1, count)]
        total = sum((part.astype(F32) for part in parts), jnp.zeros(x.shape, F32))
        return total.astype(BF16)
    total = ahead(x, axis, stride)
    upto, d = (add(x, total), 2)
    while d < count:
        part = ahead(upto, axis, stride * d)
        total, upto, d = (add(total, part), add(upto, part), 2 * d)
    return total


def prefix(keep, give, core, row):
    got = swap(give, "ctx", 1)
    low1 = jnp.where(core == 1, got, keep)
    mine, send = (add(keep[0], got[0]), add(keep[1], got[1]))
    got = swap(send, "ctx", 2)
    low2 = jnp.where(row == 1, got, mine)
    before = earlier_totals(add(mine, got), "ctx", 4)
    with_low = add(before, low2)
    got = swap(jnp.where(row == 1, before, with_low), "ctx", 2)
    before = jnp.stack([jnp.where(row == 1, with_low, before), got])
    with_low = add(before, low1)
    got = swap(jnp.where(core == 1, before, with_low), "ctx", 1)
    return jnp.where(core == 1, with_low, before), got


def on_device(queries, values, codes, codebook, out_weight):
    tokens, heads, width = queries.shape
    assert tokens == BLOCK
    devices = lax.axis_size("ctx")
    here, side = (lax.axis_index("ctx"), lax.axis_index("head"))
    sides = lax.axis_size("head")
    core, row = (here & 1, here >> 1 & 1)
    pos = jnp.stack([core, row]).astype(jnp.int32)
    lay = Layout(devices, heads, codebook.shape[1])
    codes = codes.T

    rows, columns = (out_weight.shape[0], out_weight.shape[1] // sides)
    half = rows // 2
    weights = {0: lax.dynamic_slice(out_weight, (0, side * columns), (rows, columns))}
    for k in range(1, sides):
        block = lax.dynamic_slice(out_weight, (core * half, (side ^ k) * columns), (half, columns))
        mine = swap(block, "head", k)
        other = swap(mine, "ctx", 1)
        first = core == 0
        weights[k] = jnp.stack([jnp.where(first, mine, other), jnp.where(first, other, mine)]).reshape(rows, columns)

    pieces = block_sums(lay, pos, codes, values)
    qt, num, ml = window(codes, queries, values, codebook)
    wide = lay.heads * width
    total = jnp.zeros((tokens, columns), F32)
    for g, (keep, give) in enumerate(pieces):
        mine, theirs = prefix(keep, give, core, row)
        attended = attend(lay, g, pos, qt, codebook, num, ml, mine, theirs)
        for k in range(sides):
            part = attended if k == 0 else swap(attended, "head", k)
            total = total + dot(part, weights[k][g * wide : (g + 1) * wide])
    return total.astype(BF16)


def solution(mesh):
    return jax.shard_map(
        on_device,
        mesh=mesh,
        in_specs=(
            P("ctx", "head", None),
            P("ctx", "head", None),
            P("ctx", "head"),
            P("head", None, None),
            P("head", None),
        ),
        out_specs=P("ctx", "head"),
        check_vma=False,
    )
```

```python
import functools
import math

import jax
import jax.numpy as jnp
from jax import lax
from jax.experimental import pallas as pl
from jax.experimental.pallas import tpu as pltpu
from jax.sharding import PartitionSpec as P

BLOCK = 512
LANES = 128
GROUPS = 4
NEVER = -1e30
F32 = jnp.float32
BF16 = jnp.bfloat16
VMEM = pl.BlockSpec(memory_space=pltpu.VMEM)
SMEM = pl.BlockSpec(memory_space=pltpu.SMEM)


def dot(a, b, contract=((1,), (0,))):
    return lax.dot_general(a, b, (contract, ((), ())), preferred_element_type=F32)


def one_hot(codes, ncodes):
    table = lax.broadcasted_iota(jnp.int32, (ncodes, codes.shape[1]), 0)
    return (table == codes).astype(BF16)


class Layout:
    def __init__(self, devices, first, heads, ncodes):
        self.first, self.heads = (first, heads)
        self.each = ncodes // LANES
        self.per = heads * self.each // 4
        self.shift = int(math.log2(256 // devices + 1))
        self.digits = 1
        while (1 << (self.shift * self.digits)) <= BLOCK:
            self.digits += 1
        self.sums = self.per * LANES
        self.tail = -(-self.digits * self.per // 16) * 16
        self.rows = self.sums + self.tail
        assert ncodes % LANES == 0 and heads * self.each % 4 == 0 and devices % 4 == 0

    def place(self, head, j):
        return divmod(head * self.each + j, self.per)


def group_sums(lay, core, row, codes_ref, vt_ref, buf, keep_ref, give_ref):
    line = lax.broadcasted_iota(jnp.int32, (lay.tail, LANES), 0)
    eye = lax.broadcasted_iota(jnp.int32, (LANES, LANES), 0) == lax.broadcasted_iota(jnp.int32, (LANES, LANES), 1)
    mask = (1 << lay.shift) - 1
    tails = [jnp.zeros((lay.tail, LANES), F32) for _ in range(4)]
    tokens = codes_ref.shape[1]
    ones = jnp.ones((tokens, LANES), BF16)
    for k in range(lay.heads):
        h = lay.first + k
        onehot = one_hot(codes_ref[h : h + 1, :], lay.each * LANES)
        both = dot(onehot, jnp.concatenate([vt_ref[h], ones], axis=1))
        for j in range(lay.each):
            piece, at = lay.place(k, j)
            here = slice(j * LANES, (j + 1) * LANES)
            buf[piece // 2 ^ core, piece % 2 ^ row, at * LANES : (at + 1) * LANES, :] = both[here, :LANES].astype(BF16)
            count = jnp.sum(jnp.where(eye, both[here, LANES:], 0.0), axis=0, keepdims=True).astype(jnp.int32)
            for d in range(lay.digits):
                digit = ((count >> (lay.shift * d)) & mask).astype(F32)
                tails[piece] = jnp.where(line == d * lay.per + at, digit, tails[piece])
    for piece in range(4):
        buf[piece // 2 ^ core, piece % 2 ^ row, lay.sums :, :] = tails[piece].astype(BF16)
    keep_ref[...] = buf[0]
    give_ref[...] = buf[1]


def sums_kernel(lays, turn, pos_ref, codes_ref, values_ref, *refs):
    buf = refs[-1]
    core, row = (pos_ref[0], pos_ref[1])
    if turn:
        vt_ref = refs[0]
        vt_ref[...] = jnp.swapaxes(values_ref[...], 0, 1)
        outs = refs[1:-1]
    else:
        vt_ref = values_ref
        outs = refs[:-1]
    for g, lay in enumerate(lays):
        view = buf.at[:, :, : lay.rows, :]
        group_sums(lay, core, row, codes_ref, vt_ref, view, outs[2 * g], outs[2 * g + 1])


def block_sums(lays, turn, pos, codes, values):
    heads, tokens = codes.shape
    width = values.shape[2]
    shapes = [jax.ShapeDtypeStruct((2, lay.rows, LANES), BF16) for lay in lays for _ in range(2)]
    if turn:
        shapes = [jax.ShapeDtypeStruct((heads, tokens, width), BF16)] + shapes
    some = sum(lay.heads for lay in lays)
    outs = pl.pallas_call(
        functools.partial(sums_kernel, lays, turn),
        out_shape=shapes,
        in_specs=[SMEM, VMEM, VMEM],
        out_specs=[VMEM] * len(shapes),
        scratch_shapes=[pltpu.VMEM((2, 2, max(lay.rows for lay in lays), LANES), BF16)],
        cost_estimate=pl.CostEstimate(
            flops=8 * some * tokens * lays[0].each * LANES * width, bytes_accessed=4 * tokens * heads * width, transcendentals=0
        ),
        name="block_sums",
    )(pos, codes, values)
    vt = outs[0] if turn else values
    outs = outs[1:] if turn else outs
    return vt, [(outs[2 * g], outs[2 * g + 1]) for g in range(len(lays))]


def turn_kernel(queries_ref, book_ref, qt_ref, bt_ref):
    qt_ref[...] = jnp.swapaxes(queries_ref[...], 0, 1)
    for h in range(book_ref.shape[0]):
        bt_ref[h] = book_ref[h].T


def turn_inputs(queries, book):
    tokens, heads, width = queries.shape
    return pl.pallas_call(
        turn_kernel,
        out_shape=[
            jax.ShapeDtypeStruct((heads, tokens, width), BF16),
            jax.ShapeDtypeStruct((heads, width, book.shape[1]), BF16),
        ],
        in_specs=[VMEM] * 2,
        out_specs=[VMEM] * 2,
        cost_estimate=pl.CostEstimate(flops=4000000000, bytes_accessed=8 * tokens * heads * width, transcendentals=0),
        name="turn_inputs",
    )(queries, book)


def lane_tiles(x):
    return [x[:, j : j + LANES] for j in range(0, x.shape[1], LANES)]


def window_kernel(lay, factor, codes_ref, qt_ref, vt_ref, bt_ref, num_ref, top_ref, den_ref):
    tokens = qt_ref.shape[1]
    ncodes = bt_ref.shape[2]
    tile = tokens // 2
    causal = lax.broadcasted_iota(jnp.int32, (tile, tile), 0) >= lax.broadcasted_iota(jnp.int32, (tile, tile), 1)
    for k in range(lay.heads):
        onehot = one_hot(codes_ref[lay.first + k : lay.first + k + 1, :], ncodes)
        keys = dot(bt_ref[k], onehot).astype(BF16)
        for r in range(2):
            rows = slice(r * tile, (r + 1) * tile)
            upto = slice(0, (r + 1) * tile)
            score = dot(qt_ref[k, rows, :], keys[:, upto])
            last = jnp.where(causal, score[:, r * tile :], NEVER)
            score = jnp.concatenate([score[:, :tile], last], axis=1) if r else last
            top = jnp.max(functools.reduce(jnp.maximum, lane_tiles(score)), axis=1, keepdims=True)
            top_ref[k, rows, :] = jnp.broadcast_to(top, (tile, LANES))
            weight = jnp.exp2((score - top) * factor)
            den = jnp.sum(sum(lane_tiles(weight)), axis=1, keepdims=True)
            den_ref[k, rows, :] = jnp.broadcast_to(den, (tile, LANES))
            num_ref[k, rows, :] = dot(weight.astype(BF16), vt_ref[k, upto, :])


def part_of(lay, x):
    first, count = (lay.first, lay.heads)
    assert first % count == 0
    return pl.BlockSpec((count,) + x.shape[1:], lambda i: (first // count, 0, 0))


def whole(x):
    return pl.BlockSpec(x.shape, lambda i: (0,) * len(x.shape))


def window(lay, codes, qt, vt, bt):
    heads, tokens, width = qt.shape
    factor = width ** (-0.5) * math.log2(math.e)
    shape = jax.ShapeDtypeStruct((lay.heads, tokens, width), F32)
    return pl.pallas_call(
        functools.partial(window_kernel, lay, factor),
        out_shape=[shape] * 3,
        grid=(1,),
        in_specs=[whole(codes), part_of(lay, qt), part_of(lay, vt), part_of(lay, bt)],
        out_specs=[whole(shape)] * 3,
        cost_estimate=pl.CostEstimate(flops=2400000000, bytes_accessed=18 * tokens * lay.heads * width, transcendentals=0),
        name="window",
    )(codes, qt, vt, bt)


def codes_kernel(lay, factor, pos_ref, qt_ref, bt_ref, num_ref, top_ref, den_ref, mine_ref, theirs_ref, out_ref, buf):
    core, row = (pos_ref[0], pos_ref[1])
    tokens, width = qt_ref.shape[1:]
    tile = tokens // 2
    buf[core] = mine_ref[...]
    buf[1 - core] = theirs_ref[...]
    tails = [buf[p // 2, p % 2 ^ row, lay.sums :, :].astype(F32) for p in range(4)]
    for k in range(lay.heads):
        sums, counts = ([], [])
        for j in range(lay.each):
            p, at = lay.place(k, j)
            sums.append(buf[p // 2, p % 2 ^ row, at * LANES : (at + 1) * LANES, :])
            count = 0.0
            for d in range(lay.digits):
                line = d * lay.per + at
                count = count + tails[p][line : line + 1] * float(1 << (lay.shift * d))
            counts.append(count)
        cache = jnp.concatenate(sums, axis=0)
        for r in range(2):
            rows = slice(r * tile, (r + 1) * tile)
            scores = lane_tiles(dot(qt_ref[k, rows, :], bt_ref[k]))
            scores = [s + jnp.where(n > 0.5, 0.0, NEVER) for s, n in zip(scores, counts)]
            early = top_ref[k, rows, :]
            top = jnp.maximum(early, jnp.max(functools.reduce(jnp.maximum, scores), axis=1, keepdims=True))
            weights = [jnp.exp2((s - top) * factor) for s in scores]
            keep = jnp.exp2((early - top) * factor)
            den = jnp.sum(sum(w * n for w, n in zip(weights, counts)), axis=1, keepdims=True)
            den = keep * den_ref[k, rows, :] + den
            num = dot(jnp.concatenate([w.astype(BF16) for w in weights], axis=1), cache)
            num = keep * num_ref[k, rows, :] + num
            out_ref[rows, k * width : (k + 1) * width] = (num * (1.0 / den)).astype(BF16)


def attend(lay, pos, qt, bt, num, top, den, mine, theirs):
    heads, tokens, width = qt.shape
    factor = width ** (-0.5) * math.log2(math.e)
    out = jax.ShapeDtypeStruct((tokens, lay.heads * width), BF16)
    return pl.pallas_call(
        functools.partial(codes_kernel, lay, factor),
        out_shape=out,
        grid=(1,),
        in_specs=[SMEM, part_of(lay, qt), part_of(lay, bt)] + [whole(x) for x in (num, top, den, mine, theirs)],
        out_specs=whole(out),
        scratch_shapes=[pltpu.VMEM((2, 2, lay.rows, LANES), BF16)],
        cost_estimate=pl.CostEstimate(flops=2000000000, bytes_accessed=14 * tokens * lay.heads * width, transcendentals=0),
        name="attend",
    )(pos, qt, bt, num, top, den, mine, theirs)


def mix_kernel(spans, *refs):
    n = len(spans)
    parts, weights, out_ref = (refs[:n], refs[n : 2 * n], refs[-1])
    base = refs[2 * n] if len(refs) == 2 * n + 2 else None
    tokens, columns = out_ref.shape
    wide = min(columns, 256)
    tile = tokens // 2
    for r in range(0, tokens, tile):
        for c in range(0, columns, wide):
            total = sum(dot(p[r : r + tile, :], w[a:b, c : c + wide]) for p, w, (a, b) in zip(parts, weights, spans))
            if base is not None:
                total = total + base[r : r + tile, c : c + wide]
            out_ref[r : r + tile, c : c + wide] = total.astype(out_ref.dtype)


def mix(terms, base, dtype):
    parts, weights, spans = zip(*terms)
    tokens, columns = (parts[0].shape[0], weights[0].shape[1])
    extra = [] if base is None else [base]
    return pl.pallas_call(
        functools.partial(mix_kernel, spans),
        out_shape=jax.ShapeDtypeStruct((tokens, columns), dtype),
        in_specs=[VMEM] * (2 * len(terms) + len(extra)),
        out_specs=VMEM,
        cost_estimate=pl.CostEstimate(flops=2 * tokens * columns * sum(p.shape[1] for p in parts), bytes_accessed=8 * tokens * columns, transcendentals=0),
        name="mix",
    )(*parts, *weights, *extra)


def swap(x, axis, k):
    return lax.ppermute(x, axis, [(i, i ^ k) for i in range(lax.axis_size(axis))])


def add(a, b):
    return (a.astype(F32) + b.astype(F32)).astype(BF16)


def prefix(keep, give, here):
    upper = lambda bit: (here & bit) != 0
    got1 = swap(give, "ctx", 1)
    mine, send = (add(keep[0], got1[0]), add(keep[1], got1[1]))
    got2 = swap(send, "ctx", 2)
    total = add(mine, got2)
    before = jnp.zeros_like(total)
    bit = 4
    while bit < lax.axis_size("ctx"):
        got = swap(total, "ctx", bit)
        before = jnp.where(upper(bit), add(before, got), before)
        total = add(total, got)
        bit *= 2
    with_low = add(before, jnp.where(upper(2), got2, mine))
    got = swap(jnp.where(upper(2), before, with_low), "ctx", 2)
    before = jnp.stack([jnp.where(upper(2), with_low, before), got])
    with_low = add(before, jnp.where(upper(1), got1, keep))
    got = swap(jnp.where(upper(1), before, with_low), "ctx", 1)
    return jnp.where(upper(1), with_low, before), got


def on_device(queries, values, codes, codebook, out_weight):
    tokens, heads, width = queries.shape
    assert tokens == BLOCK
    devices = lax.axis_size("ctx")
    assert devices & (devices - 1) == 0
    here, side = (lax.axis_index("ctx"), lax.axis_index("head"))
    sides = lax.axis_size("head")
    core, row = (here & 1, here >> 1 & 1)
    pos = jnp.stack([core, row]).astype(jnp.int32)
    count = heads // math.gcd(GROUPS, heads)
    lays = [Layout(devices, first, count, codebook.shape[1]) for first in range(0, heads, count)]
    codes = codes.T

    rows, columns = (out_weight.shape[0], out_weight.shape[1] // sides)
    half = rows // 2
    weights = {0: lax.dynamic_slice(out_weight, (0, side * columns), (rows, columns))}
    for k in range(1, sides):
        block = lax.dynamic_slice(out_weight, (core * half, (side ^ k) * columns), (half, columns))
        mine = swap(block, "head", k)
        other = swap(mine, "ctx", 1)
        first = core == 0
        weights[k] = jnp.stack([jnp.where(first, mine, other), jnp.where(first, other, mine)]).reshape(rows, columns)

    vt, pieces = block_sums(lays[:1], True, pos, codes, values)
    if lays[1:]:
        pieces += block_sums(lays[1:], False, pos, codes, vt)[1]
    qt, bt = turn_inputs(queries, codebook)
    wide = count * width
    terms = []
    for g, (lay, (keep, give)) in enumerate(zip(lays, pieces)):
        num, top, den = window(lay, codes, qt, vt, bt)
        mine, theirs = prefix(keep, give, here)
        attended = attend(lay, pos, qt, bt, num, top, den, mine, theirs)
        span = (g * wide, (g + 1) * wide)
        terms.append((attended, weights[0], span))
        terms += [(swap(attended, "head", k), weights[k], span) for k in range(1, sides)]
    late = len(terms) - (sides - 1)
    return mix(terms[late:], mix(terms[:late], None, F32), BF16)


def solution(mesh):
    return jax.shard_map(
        on_device,
        mesh=mesh,
        in_specs=(
            P("ctx", "head", None),
            P("ctx", "head", None),
            P("ctx", "head"),
            P("head", None, None),
            P("head", None),
        ),
        out_specs=P("ctx", "head"),
        check_vma=False,
    )
```

```python
import functools
import math

import jax
import jax.numpy as jnp
from jax import lax
from jax.experimental import pallas as pl
from jax.experimental.pallas import tpu as pltpu
from jax.sharding import PartitionSpec as P

BLOCK = 512
LANES = 128
SIZES = (2, 2, 2, 2)
LIMIT = 20 << 20
NEVER = -1e30
F32 = jnp.float32
BF16 = jnp.bfloat16
VMEM = pl.BlockSpec(memory_space=pltpu.VMEM)
SMEM = pl.BlockSpec(memory_space=pltpu.SMEM)
ANY = pl.BlockSpec(memory_space=pl.ANY)
PARAMS = pltpu.CompilerParams(vmem_limit_bytes=LIMIT)


def dot(a, b, contract=((1,), (0,))):
    return lax.dot_general(a, b, (contract, ((), ())), preferred_element_type=F32)


def one_hot(codes, ncodes):
    table = lax.broadcasted_iota(jnp.int32, (ncodes, codes.shape[1]), 0)
    return (table == codes).astype(BF16)


class Layout:
    def __init__(self, devices, first, heads, ncodes):
        self.first, self.heads = (first, heads)
        self.each = ncodes // LANES
        self.per = heads * self.each // 4
        self.shift = int(math.log2(256 // devices + 1))
        self.digits = 1
        while (1 << (self.shift * self.digits)) <= BLOCK:
            self.digits += 1
        self.sums = self.per * LANES
        self.tail = -(-self.digits * self.per // 16) * 16
        self.rows = self.sums + self.tail
        assert ncodes % LANES == 0 and heads * self.each % 4 == 0 and devices % 4 == 0

    def place(self, head, j):
        return divmod(head * self.each + j, self.per)


def group_sums(lay, core, row, codes_ref, vt_ref, buf, keep_ref, give_ref):
    line = lax.broadcasted_iota(jnp.int32, (lay.tail, LANES), 0)
    eye = lax.broadcasted_iota(jnp.int32, (LANES, LANES), 0) == lax.broadcasted_iota(jnp.int32, (LANES, LANES), 1)
    mask = (1 << lay.shift) - 1
    tails = [jnp.zeros((lay.tail, LANES), F32) for _ in range(4)]
    tokens = codes_ref.shape[1]
    ones = jnp.ones((tokens, LANES), BF16)
    for k in range(lay.heads):
        h = lay.first + k
        onehot = one_hot(codes_ref[h : h + 1, :], lay.each * LANES)
        both = dot(onehot, jnp.concatenate([vt_ref[h], ones], axis=1))
        for j in range(lay.each):
            piece, at = lay.place(k, j)
            here = slice(j * LANES, (j + 1) * LANES)
            buf[piece // 2 ^ core, piece % 2 ^ row, at * LANES : (at + 1) * LANES, :] = both[here, :LANES].astype(BF16)
            count = jnp.sum(jnp.where(eye, both[here, LANES:], 0.0), axis=0, keepdims=True).astype(jnp.int32)
            for d in range(lay.digits):
                digit = ((count >> (lay.shift * d)) & mask).astype(F32)
                tails[piece] = jnp.where(line == d * lay.per + at, digit, tails[piece])
    for piece in range(4):
        buf[piece // 2 ^ core, piece % 2 ^ row, lay.sums :, :] = tails[piece].astype(BF16)
    keep_ref[...] = buf[0]
    give_ref[...] = buf[1]


def sums_kernel(lays, turn, pos_ref, codes_ref, values_ref, *refs):
    buf = refs[-1]
    core, row = (pos_ref[0], pos_ref[1])
    if turn:
        vt_ref = refs[0]
        vt_ref[...] = jnp.swapaxes(values_ref[...], 0, 1)
        outs = refs[1:-1]
    else:
        vt_ref = values_ref
        outs = refs[:-1]
    for g, lay in enumerate(lays):
        view = buf.at[:, :, : lay.rows, :]
        group_sums(lay, core, row, codes_ref, vt_ref, view, outs[2 * g], outs[2 * g + 1])


def block_sums(lays, turn, pos, codes, values):
    heads, tokens = codes.shape
    width = values.shape[2]
    shapes = [jax.ShapeDtypeStruct((2, lay.rows, LANES), BF16) for lay in lays for _ in range(2)]
    if turn:
        shapes = [jax.ShapeDtypeStruct((heads, tokens, width), BF16)] + shapes
    some = sum(lay.heads for lay in lays)
    outs = pl.pallas_call(
        functools.partial(sums_kernel, lays, turn),
        out_shape=shapes,
        in_specs=[SMEM, VMEM, VMEM],
        out_specs=[VMEM] * len(shapes),
        scratch_shapes=[pltpu.VMEM((2, 2, max(lay.rows for lay in lays), LANES), BF16)],
        compiler_params=PARAMS,
        cost_estimate=pl.CostEstimate(
            flops=8 * some * tokens * lays[0].each * LANES * width, bytes_accessed=4 * tokens * heads * width, transcendentals=0
        ),
        name="block_sums",
    )(pos, codes, values)
    vt = outs[0] if turn else values
    outs = outs[1:] if turn else outs
    return vt, [(outs[2 * g], outs[2 * g + 1]) for g in range(len(lays))]


def turn_kernel(after_ref, queries_ref, book_ref, qt_ref, bt_ref):
    del after_ref
    qt_ref[...] = jnp.swapaxes(queries_ref[...], 0, 1)
    for h in range(book_ref.shape[0]):
        bt_ref[h] = book_ref[h].T


def turn_inputs(after, queries, book):
    tokens, heads, width = queries.shape
    return pl.pallas_call(
        turn_kernel,
        out_shape=[
            jax.ShapeDtypeStruct((heads, tokens, width), BF16),
            jax.ShapeDtypeStruct((heads, width, book.shape[1]), BF16),
        ],
        in_specs=[ANY, VMEM, VMEM],
        out_specs=[VMEM] * 2,
        compiler_params=PARAMS,
        cost_estimate=pl.CostEstimate(flops=4000000000, bytes_accessed=8 * tokens * heads * width, transcendentals=0),
        name="turn_inputs",
    )(after, queries, book)


def lane_tiles(x):
    return [x[:, j : j + LANES] for j in range(0, x.shape[1], LANES)]


def window_kernel(lay, factor, after_ref, codes_ref, qt_ref, vt_ref, bt_ref, num_ref, top_ref, den_ref):
    del after_ref
    tokens = qt_ref.shape[1]
    ncodes = bt_ref.shape[2]
    tile = tokens // 2
    causal = lax.broadcasted_iota(jnp.int32, (tile, tile), 0) >= lax.broadcasted_iota(jnp.int32, (tile, tile), 1)
    for k in range(lay.heads):
        h = lay.first + k
        onehot = one_hot(codes_ref[h : h + 1, :], ncodes)
        keys = dot(bt_ref[h], onehot).astype(BF16)
        for r in range(2):
            rows = slice(r * tile, (r + 1) * tile)
            upto = slice(0, (r + 1) * tile)
            score = dot(qt_ref[h, rows, :], keys[:, upto])
            last = jnp.where(causal, score[:, r * tile :], NEVER)
            score = jnp.concatenate([score[:, :tile], last], axis=1) if r else last
            top = jnp.max(functools.reduce(jnp.maximum, lane_tiles(score)), axis=1, keepdims=True)
            top_ref[k, rows, :] = jnp.broadcast_to(top, (tile, LANES))
            weight = jnp.exp2((score - top) * factor)
            den = jnp.sum(sum(lane_tiles(weight)), axis=1, keepdims=True)
            den_ref[k, rows, :] = jnp.broadcast_to(den, (tile, LANES))
            num_ref[k, rows, :] = dot(weight.astype(BF16), vt_ref[h, upto, :])


def window(lay, after, codes, qt, vt, bt):
    heads, tokens, width = qt.shape
    factor = width ** (-0.5) * math.log2(math.e)
    shape = jax.ShapeDtypeStruct((lay.heads, tokens, width), F32)
    return pl.pallas_call(
        functools.partial(window_kernel, lay, factor),
        out_shape=[shape] * 3,
        in_specs=[ANY] + [VMEM] * 4,
        out_specs=[VMEM] * 3,
        compiler_params=PARAMS,
        cost_estimate=pl.CostEstimate(flops=2400000000, bytes_accessed=18 * tokens * lay.heads * width, transcendentals=0),
        name="window",
    )(after, codes, qt, vt, bt)


def codes_kernel(lay, factor, pos_ref, qt_ref, bt_ref, num_ref, top_ref, den_ref, mine_ref, theirs_ref, out_ref, buf):
    core, row = (pos_ref[0], pos_ref[1])
    tokens, width = qt_ref.shape[1:]
    tile = tokens // 2
    buf[core] = mine_ref[...]
    buf[1 - core] = theirs_ref[...]
    tails = [buf[p // 2, p % 2 ^ row, lay.sums :, :].astype(F32) for p in range(4)]
    for k in range(lay.heads):
        sums, counts = ([], [])
        for j in range(lay.each):
            p, at = lay.place(k, j)
            sums.append(buf[p // 2, p % 2 ^ row, at * LANES : (at + 1) * LANES, :])
            count = 0.0
            for d in range(lay.digits):
                line = d * lay.per + at
                count = count + tails[p][line : line + 1] * float(1 << (lay.shift * d))
            counts.append(count)
        cache = jnp.concatenate(sums, axis=0)
        for r in range(2):
            rows = slice(r * tile, (r + 1) * tile)
            scores = lane_tiles(dot(qt_ref[lay.first + k, rows, :], bt_ref[lay.first + k]))
            scores = [s + jnp.where(n > 0.5, 0.0, NEVER) for s, n in zip(scores, counts)]
            early = top_ref[k, rows, :]
            top = jnp.maximum(early, jnp.max(functools.reduce(jnp.maximum, scores), axis=1, keepdims=True))
            weights = [jnp.exp2((s - top) * factor) for s in scores]
            keep = jnp.exp2((early - top) * factor)
            den = jnp.sum(sum(w * n for w, n in zip(weights, counts)), axis=1, keepdims=True)
            den = keep * den_ref[k, rows, :] + den
            num = dot(jnp.concatenate([w.astype(BF16) for w in weights], axis=1), cache)
            num = keep * num_ref[k, rows, :] + num
            out_ref[rows, k * width : (k + 1) * width] = (num * (1.0 / den)).astype(BF16)


def attend(lay, pos, qt, bt, num, top, den, mine, theirs):
    heads, tokens, width = qt.shape
    factor = width ** (-0.5) * math.log2(math.e)
    out = jax.ShapeDtypeStruct((tokens, lay.heads * width), BF16)
    return pl.pallas_call(
        functools.partial(codes_kernel, lay, factor),
        out_shape=out,
        in_specs=[SMEM] + [VMEM] * 7,
        out_specs=VMEM,
        scratch_shapes=[pltpu.VMEM((2, 2, lay.rows, LANES), BF16)],
        compiler_params=PARAMS,
        cost_estimate=pl.CostEstimate(flops=2000000000, bytes_accessed=14 * tokens * lay.heads * width, transcendentals=0),
        name="attend",
    )(pos, qt, bt, num, top, den, mine, theirs)


def mix_kernel(terms, parts, extra, *refs):
    weights, out_ref = (refs[parts:-1], refs[-1])
    tokens, columns = out_ref.shape
    wide = min(columns, 256)
    tile = tokens // 2
    for r in range(0, tokens, tile):
        for c in range(0, columns, wide):
            total = sum(
                dot(refs[n][r : r + tile, :], weights[w][a:b, c : c + wide]) for n, (w, a, b) in enumerate(terms)
            )
            if extra:
                total = total + refs[-2][r : r + tile, c : c + wide]
            out_ref[r : r + tile, c : c + wide] = total.astype(out_ref.dtype)


def mix(terms, weights, base, dtype):
    parts = [term[0] for term in terms]
    used = sorted({term[1] for term in terms})
    spans = [(used.index(w), a, b) for _, w, a, b in terms]
    tokens, columns = (parts[0].shape[0], weights[0].shape[1])
    extra = [] if base is None else [base]
    return pl.pallas_call(
        functools.partial(mix_kernel, spans, len(parts), len(extra)),
        out_shape=jax.ShapeDtypeStruct((tokens, columns), dtype),
        in_specs=[VMEM] * (len(parts) + len(used) + len(extra)),
        out_specs=VMEM,
        compiler_params=PARAMS,
        cost_estimate=pl.CostEstimate(
            flops=2 * tokens * columns * sum(p.shape[1] for p in parts), bytes_accessed=8 * tokens * columns, transcendentals=0
        ),
        name="mix",
    )(*parts, *[weights[w] for w in used], *extra)


def swap(x, axis, k):
    return lax.ppermute(x, axis, [(i, i ^ k) for i in range(lax.axis_size(axis))])


def add(a, b):
    return (a.astype(F32) + b.astype(F32)).astype(BF16)


class Prefix:
    def __init__(self, keep, give, here):
        self.keep, self.here = (keep, here)
        self.got1 = swap(give, "ctx", 1)

    def upper(self, bit):
        return (self.here & bit) != 0

    def reduce(self):
        keep, got1 = (self.keep, self.got1)
        self.mine, send = (add(keep[0], got1[0]), add(keep[1], got1[1]))
        self.got2 = swap(send, "ctx", 2)
        return send

    def start(self):
        self.total = add(self.mine, self.got2)
        self.before = jnp.zeros_like(self.total)

    def step(self, bit):
        sent = self.total
        got = swap(sent, "ctx", bit)
        self.before = jnp.where(self.upper(bit), add(self.before, got), self.before)
        self.total = add(self.total, got)
        return sent

    def spread(self):
        before, got2 = (self.before, self.got2)
        with_low = add(before, jnp.where(self.upper(2), got2, self.mine))
        got = swap(jnp.where(self.upper(2), before, with_low), "ctx", 2)
        self.before = jnp.stack([jnp.where(self.upper(2), with_low, before), got])

    def finish(self):
        before, got1 = (self.before, self.got1)
        with_low = add(before, jnp.where(self.upper(1), got1, self.keep))
        got = swap(jnp.where(self.upper(1), before, with_low), "ctx", 1)
        return jnp.where(self.upper(1), with_low, before), got


def group_sizes(heads):
    total = sum(SIZES)
    ends = [max(n + 1, heads * sum(SIZES[: n + 1]) // total) for n in range(len(SIZES))]
    ends = sorted({min(end, heads) for end in ends})
    return [b - a for a, b in zip([0] + ends, ends)]


def on_device(queries, values, codes, codebook, out_weight):
    tokens, heads, width = queries.shape
    assert tokens == BLOCK
    devices = lax.axis_size("ctx")
    assert devices & (devices - 1) == 0
    here, side = (lax.axis_index("ctx"), lax.axis_index("head"))
    sides = lax.axis_size("head")
    core, row = (here & 1, here >> 1 & 1)
    pos = jnp.stack([core, row]).astype(jnp.int32)
    lays, first = ([], 0)
    for count in group_sizes(heads):
        lays.append(Layout(devices, first, count, codebook.shape[1]))
        first += count
    codes = codes.T

    vt, pieces = block_sums(lays[:1], True, pos, codes, values)
    runs = [Prefix(*pieces[0], here)]
    if lays[1:]:
        runs += [Prefix(*piece, here) for piece in block_sums(lays[1:], False, pos, codes, vt)[1]]

    rows, columns = (out_weight.shape[0], out_weight.shape[1] // sides)
    half = rows // 2
    weights = {0: lax.dynamic_slice(out_weight, (0, side * columns), (rows, columns))}
    for k in range(1, sides):
        block = lax.dynamic_slice(out_weight, (core * half, (side ^ k) * columns), (half, columns))
        mine = swap(block, "head", k)
        other = swap(mine, "ctx", 1)
        first = core == 0
        weights[k] = jnp.stack([jnp.where(first, mine, other), jnp.where(first, other, mine)]).reshape(rows, columns)

    sent = [run.reduce() for run in runs]
    qt, bt = turn_inputs(sent[-1], queries, codebook)
    for run in runs:
        run.start()
    bit = 4
    while bit < devices:
        sent = [run.step(bit) for run in runs]
        bit *= 2
    windows = [window(lay, sent[0], codes, qt, vt, bt) for lay in lays]
    for run in runs:
        run.spread()
    terms = []
    for lay, run, (num, top, den) in zip(lays, runs, windows):
        mine, theirs = run.finish()
        attended = attend(lay, pos, qt, bt, num, top, den, mine, theirs)
        span = (lay.first * width, (lay.first + lay.heads) * width)
        terms.append((attended, 0, *span))
        terms += [(swap(attended, "head", k), k, *span) for k in range(1, sides)]
    late = len(terms) - (sides - 1)
    base = mix(terms[:late], weights, None, F32)
    return mix(terms[late:], weights, base, BF16)


def solution(mesh):
    return jax.shard_map(
        on_device,
        mesh=mesh,
        in_specs=(
            P("ctx", "head", None),
            P("ctx", "head", None),
            P("ctx", "head"),
            P("head", None, None),
            P("head", None),
        ),
        out_specs=P("ctx", "head"),
        check_vma=False,
    )
```

```python
import functools
import math

import jax
import jax.numpy as jnp
from jax import lax
from jax.experimental import pallas as pl
from jax.experimental.pallas import tpu as pltpu
from jax.sharding import PartitionSpec as P

BLOCK = 512
LANES = 128
SIZES = (2, 2, 2, 2)
LIMIT = 20 << 20
NEVER = -1e30
F32 = jnp.float32
BF16 = jnp.bfloat16
VMEM = pl.BlockSpec(memory_space=pltpu.VMEM)
ANY = pl.BlockSpec(memory_space=pl.ANY)
HBM = pl.BlockSpec(memory_space=pltpu.HBM)
PARAMS = pltpu.CompilerParams(vmem_limit_bytes=LIMIT)


def dot(a, b, contract=((1,), (0,))):
    return lax.dot_general(a, b, (contract, ((), ())), preferred_element_type=F32)


def one_hot(codes, ncodes):
    table = lax.broadcasted_iota(jnp.int32, (ncodes, codes.shape[1]), 0)
    return (table == codes).astype(BF16)


class Layout:
    def __init__(self, devices, first, heads, ncodes):
        self.first, self.heads, self.half = (first, heads, heads // 2)
        self.each = ncodes // LANES
        self.per = self.half * self.each // 2
        self.shift = int(math.log2(256 // devices + 1))
        self.digits = 1
        while (1 << (self.shift * self.digits)) <= BLOCK:
            self.digits += 1
        self.sums = self.per * LANES
        self.tail = -(-self.digits * self.per // 16) * 16
        self.rows = self.sums + self.tail
        assert ncodes % (2 * LANES) == 0 and heads % 2 == 0 and devices % 4 == 0

    def place(self, k, j):
        piece, at = divmod(j, self.each // 2)
        return (piece, k * (self.each // 2) + at)


class Chain:
    def __init__(self):
        self.last = None

    def __call__(self, kernel, shapes, args, in_hbm=(), scratch=(), name=None, flops=1000000000):
        first = [] if self.last is None else [self.last]

        def run(*refs):
            return kernel(*refs[len(first) :])

        outs = pl.pallas_call(
            run,
            out_shape=shapes,
            in_specs=[ANY] * len(first) + [HBM if n in in_hbm else VMEM for n in range(len(args))],
            out_specs=jax.tree.map(lambda _: VMEM, shapes),
            scratch_shapes=list(scratch),
            compiler_params=PARAMS,
            cost_estimate=pl.CostEstimate(flops=flops, bytes_accessed=1000000, transcendentals=0),
            name=name,
        )(*first, *args)
        self.last = jax.tree.leaves(outs)[0]
        return outs


def bit_of(bit):
    return (lax.axis_index("ctx") & bit) != 0


def shape_of(*dims, dtype=BF16):
    return jax.ShapeDtypeStruct(dims, dtype)


def turn(chain, queries, values, book, out_weight):
    tokens, heads, width = queries.shape
    sides = lax.axis_size("head")
    rows, columns = (out_weight.shape[0], out_weight.shape[1] // sides)
    half = rows // 2
    peers = range(1, sides)

    def kernel(queries_ref, values_ref, book_ref, weight_ref, vt_ref, qt_ref, bt_ref, *refs):
        blocks, sems = (refs[:-1], refs[-1])
        core, side = (lax.axis_index("ctx") & 1, lax.axis_index("head"))
        copies = []
        for n, k in enumerate(peers):
            part = weight_ref.at[
                pl.ds(pl.multiple_of(core * half, half), half), pl.ds(pl.multiple_of((side ^ k) * columns, columns), columns)
            ]
            copies.append(pltpu.make_async_copy(part, blocks[n], sems.at[n]))
            copies[-1].start()
        vt_ref[...] = jnp.swapaxes(values_ref[...], 0, 1)
        qt_ref[...] = jnp.swapaxes(queries_ref[...], 0, 1)
        for h in range(heads):
            bt_ref[h] = book_ref[h].T
        for copy in copies:
            copy.wait()

    shapes = [shape_of(heads, tokens, width), shape_of(heads, tokens, width), shape_of(heads, width, book.shape[1])]
    shapes += [shape_of(half, columns) for _ in peers]
    outs = chain(
        kernel, shapes, (queries, values, book, out_weight), in_hbm=(3,),
        scratch=[pltpu.SemaphoreType.DMA((max(1, len(peers)),))], name="turn",
    )
    return outs[0], outs[1], outs[2], outs[3:]


def block_sums(chain, lay, codes, codes2, vt, values2, turned):
    heads, tokens = codes.shape

    def kernel(codes_ref, codes2_ref, vt_ref, values2_ref, mine_ref, send_ref, low_ref, *refs):
        buf = refs[-1]
        if turned:
            vt2_ref = values2_ref
        else:
            vt2_ref = refs[0]
            vt2_ref[...] = jnp.swapaxes(values2_ref[...], 0, 1)
        core, row = (bit_of(1), bit_of(2).astype(jnp.int32))
        line = lax.broadcasted_iota(jnp.int32, (lay.tail, LANES), 0)
        eye = lax.broadcasted_iota(jnp.int32, (LANES, LANES), 0) == lax.broadcasted_iota(jnp.int32, (LANES, LANES), 1)
        mask = (1 << lay.shift) - 1
        ones = jnp.ones((tokens, LANES), BF16)
        tails = [[jnp.zeros((lay.tail, LANES), F32) for _ in range(2)] for _ in range(2)]
        for k in range(lay.half):
            h = lay.first + core.astype(jnp.int32) * lay.half + k
            own, other = [
                dot(one_hot(c[pl.ds(h, 1), :], lay.each * LANES), jnp.concatenate([v[h], ones], axis=1))
                for c, v in ((codes_ref, vt_ref), (codes2_ref, vt2_ref))
            ]
            for to, ref, both in ((0, buf, own + other), (1, low_ref, jnp.where(core, other, own))):
                for j in range(lay.each):
                    piece, at = lay.place(k, j)
                    here = slice(j * LANES, (j + 1) * LANES)
                    ref[piece ^ row, at * LANES : (at + 1) * LANES, :] = both[here, :LANES].astype(BF16)
                    count = jnp.sum(jnp.where(eye, both[here, LANES:], 0.0), axis=0, keepdims=True).astype(jnp.int32)
                    for d in range(lay.digits):
                        digit = ((count >> (lay.shift * d)) & mask).astype(F32)
                        tails[to][piece] = jnp.where(line == d * lay.per + at, digit, tails[to][piece])
        for to, ref in ((0, buf), (1, low_ref)):
            for piece in range(2):
                ref[piece ^ row, lay.sums :, :] = tails[to][piece].astype(BF16)
        mine_ref[...] = buf[0]
        send_ref[...] = buf[1]

    shapes = [shape_of(lay.rows, LANES)] * 2 + [shape_of(2, lay.rows, LANES)]
    if not turned:
        shapes.append(shape_of(*vt.shape))
    return chain(
        kernel, shapes, (codes, codes2, vt, values2), scratch=[pltpu.VMEM((2, lay.rows, LANES), BF16)], name="block_sums"
    )


def plus(chain, a, b):
    def kernel(a_ref, b_ref, out_ref):
        out_ref[...] = (a_ref[...].astype(F32) + b_ref[...].astype(F32)).astype(BF16)

    return chain(kernel, shape_of(*a.shape), (a, b), name="plus")


def with_low(before, low, flag):
    more = (before + low.astype(F32)).astype(BF16)
    before = before.astype(BF16)
    return jnp.where(flag, more, before), jnp.where(flag, before, more)


def spread(chain, got, bits, got2, mine):
    def kernel(*refs):
        got_refs, (got2_ref, mine_ref, own_ref, send_ref) = (refs[:-4], refs[-4:])
        before = 0.0
        for ref, bit in zip(got_refs, bits):
            before = before + jnp.where(bit_of(bit), ref[...].astype(F32), 0.0)
        low = jnp.where(bit_of(2), got2_ref[...].astype(F32), mine_ref[...].astype(F32))
        own_ref[...], send_ref[...] = with_low(before, low, bit_of(2))

    return chain(kernel, [shape_of(*mine.shape)] * 2, (*got, got2, mine), name="spread")


def share(chain, own, got, low):
    def kernel(own_ref, got_ref, low_ref, mine_ref, send_ref):
        for n, ref in enumerate((own_ref, got_ref)):
            mine_ref[n], send_ref[n] = with_low(ref[...].astype(F32), low_ref[n], bit_of(1))

    return chain(kernel, [shape_of(*low.shape)] * 2, (own, got, low), name="share")


def lane_tiles(x):
    return [x[:, j : j + LANES] for j in range(0, x.shape[1], LANES)]


def window(chain, lay, codes, qt, vt, bt, out_weight=None):
    heads, tokens, width = qt.shape
    factor = width ** (-0.5) * math.log2(math.e)
    tile = tokens // 2
    columns = out_weight.shape[1] // lax.axis_size("head") if out_weight is not None else 0

    def kernel(codes_ref, qt_ref, vt_ref, bt_ref, *refs):
        if columns:
            weight_ref, num_ref, top_ref, den_ref, own_ref, sem = refs
            at = pl.multiple_of(lax.axis_index("head") * columns, columns)
            copy = pltpu.make_async_copy(weight_ref.at[:, pl.ds(at, columns)], own_ref, sem.at[0])
            copy.start()
        else:
            num_ref, top_ref, den_ref = refs
        causal = lax.broadcasted_iota(jnp.int32, (tile, tile), 0) >= lax.broadcasted_iota(jnp.int32, (tile, tile), 1)
        for k in range(lay.heads):
            h = lay.first + k
            keys = dot(bt_ref[h], one_hot(codes_ref[h : h + 1, :], bt_ref.shape[2])).astype(BF16)
            for r in range(2):
                rows = slice(r * tile, (r + 1) * tile)
                upto = slice(0, (r + 1) * tile)
                score = dot(qt_ref[h, rows, :], keys[:, upto])
                last = jnp.where(causal, score[:, r * tile :], NEVER)
                score = jnp.concatenate([score[:, :tile], last], axis=1) if r else last
                top = jnp.max(functools.reduce(jnp.maximum, lane_tiles(score)), axis=1, keepdims=True)
                top_ref[k, rows, :] = jnp.broadcast_to(top, (tile, LANES))
                weight = jnp.exp2((score - top) * factor)
                den = jnp.sum(sum(lane_tiles(weight)), axis=1, keepdims=True)
                den_ref[k, rows, :] = jnp.broadcast_to(den, (tile, LANES))
                num_ref[k, rows, :] = dot(weight.astype(BF16), vt_ref[h, upto, :])
        if columns:
            copy.wait()

    shapes = [shape_of(lay.heads, tokens, n, dtype=F32) for n in (width, LANES, LANES)]
    args, scratch = ([codes, qt, vt, bt], [])
    if columns:
        args.append(out_weight)
        shapes.append(shape_of(out_weight.shape[0], columns))
        scratch = [pltpu.SemaphoreType.DMA((1,))]
    return chain(kernel, shapes, args, in_hbm=(4,), scratch=scratch, name="window", flops=200000000)


def attend(chain, lay, qt, bt, num, top, den, mine, theirs):
    heads, tokens, width = qt.shape
    factor = width ** (-0.5) * math.log2(math.e)
    tile = tokens // 2

    def kernel(qt_ref, bt_ref, num_ref, top_ref, den_ref, mine_ref, theirs_ref, out_ref, buf):
        core, row = (bit_of(1).astype(jnp.int32), bit_of(2).astype(jnp.int32))
        buf[core] = mine_ref[...]
        buf[1 - core] = theirs_ref[...]
        tails = [[buf[c, p ^ row, lay.sums :, :].astype(F32) for p in range(2)] for c in range(2)]
        for k in range(lay.heads):
            h = lay.first + k
            owner, within = divmod(k, lay.half)
            sums, counts = ([], [])
            for j in range(lay.each):
                p, at = lay.place(within, j)
                sums.append(buf[owner, p ^ row, at * LANES : (at + 1) * LANES, :])
                count = 0.0
                for d in range(lay.digits):
                    line = d * lay.per + at
                    count = count + tails[owner][p][line : line + 1] * float(1 << (lay.shift * d))
                counts.append(count)
            cache = jnp.concatenate(sums, axis=0)
            for r in range(2):
                rows = slice(r * tile, (r + 1) * tile)
                scores = lane_tiles(dot(qt_ref[h, rows, :], bt_ref[h]))
                scores = [s + jnp.where(n > 0.5, 0.0, NEVER) for s, n in zip(scores, counts)]
                early = top_ref[k, rows, :]
                top = jnp.maximum(early, jnp.max(functools.reduce(jnp.maximum, scores), axis=1, keepdims=True))
                weights = [jnp.exp2((s - top) * factor) for s in scores]
                keep = jnp.exp2((early - top) * factor)
                den = jnp.sum(sum(w * n for w, n in zip(weights, counts)), axis=1, keepdims=True)
                den = keep * den_ref[k, rows, :] + den
                num = dot(jnp.concatenate([w.astype(BF16) for w in weights], axis=1), cache)
                num = keep * num_ref[k, rows, :] + num
                out_ref[rows, k * width : (k + 1) * width] = (num * (1.0 / den)).astype(BF16)

    return chain(
        kernel, shape_of(tokens, lay.heads * width), (qt, bt, num, top, den, mine, theirs),
        scratch=[pltpu.VMEM((2, 2, lay.rows, LANES), BF16)], name="attend",
    )


def mix(chain, terms, weights, base, dtype):
    parts = [term[0] for term in terms]
    used = sorted({term[1] for term in terms})
    spans = [(used.index(w), a, b) for _, w, a, b in terms]
    tokens, columns = (parts[0].shape[0], weights[0].shape[1])
    extra = [] if base is None else [base]
    wide, tile = (min(columns, 256), tokens // 2)

    def kernel(*refs):
        out_ref = refs[-1]
        for r in range(0, tokens, tile):
            for c in range(0, columns, wide):
                total = sum(
                    dot(refs[n][r : r + tile, :], refs[len(parts) + w][a:b, c : c + wide])
                    for n, (w, a, b) in enumerate(spans)
                )
                if extra:
                    total = total + refs[-2][r : r + tile, c : c + wide]
                out_ref[r : r + tile, c : c + wide] = total.astype(out_ref.dtype)

    return chain(kernel, shape_of(tokens, columns, dtype=dtype), (*parts, *[weights[w] for w in used], *extra), name="mix")


def swap(x, axis, k):
    return lax.ppermute(x, axis, [(i, i ^ k) for i in range(lax.axis_size(axis))])


def group_sizes(heads):
    ends = [max(n + 1, heads // 2 * sum(SIZES[: n + 1]) // sum(SIZES)) for n in range(len(SIZES))]
    ends = sorted({min(end, heads // 2) for end in ends})
    return [2 * (b - a) for a, b in zip([0] + ends, ends)]


def on_device(queries, values, codes, codebook, out_weight):
    tokens, heads, width = queries.shape
    assert tokens == BLOCK
    devices, sides = (lax.axis_size("ctx"), lax.axis_size("head"))
    assert devices & (devices - 1) == 0 and sides & (sides - 1) == 0
    lays, first = ([], 0)
    for count in group_sizes(heads):
        lays.append(Layout(devices, first, count, codebook.shape[1]))
        first += count
    codes = codes.T
    chain = Chain()

    values2, codes2 = (swap(values, "ctx", 1), swap(codes, "ctx", 1))
    vt, qt, bt, blocks = turn(chain, queries, values, codebook, out_weight)
    blocks = [swap(block, "head", k + 1) for k, block in enumerate(blocks)]

    runs = []
    for n, lay in enumerate(lays):
        outs = block_sums(chain, lay, codes, codes2, vt, values2, n > 0)
        if n == 0:
            values2 = outs[3]
        runs.append((*outs[:3], swap(outs[1], "ctx", 2)))
    totals = []
    for mine, send, low, got2 in runs:
        totals.append(plus(chain, mine, got2))
    bits = [1 << n for n in range(2, devices.bit_length() - 1)]
    windows = [window(chain, lays[0], codes, qt, vt, bt, out_weight)]
    got = [[] for _ in runs]
    for bit in bits:
        arrived = [swap(total, "ctx", bit) for total in totals]
        for g, part in enumerate(arrived):
            got[g].append(part)
        if bit != bits[-1]:
            totals = [plus(chain, total, part) for total, part in zip(totals, arrived)]
    windows += [window(chain, lay, codes, qt, vt, bt) for lay in lays[1:]]
    pairs = [spread(chain, got[g], bits, run[3], run[0]) for g, run in enumerate(runs)]
    pairs = [(own, swap(send, "ctx", 2)) for own, send in pairs]
    pairs = [share(chain, own, other, run[2]) for run, (own, other) in zip(runs, pairs)]
    pairs = [(mine, swap(send, "ctx", 1)) for mine, send in pairs]

    weights = {0: windows[0][3]}
    core = lax.axis_index("ctx") & 1
    for k, mine in enumerate(blocks):
        other = swap(mine, "ctx", 1)
        both = jnp.stack([jnp.where(core == 0, mine, other), jnp.where(core == 0, other, mine)])
        weights[k + 1] = both.reshape(-1, mine.shape[1])
    terms = []
    for lay, pair, (num, top, den, *_) in zip(lays, pairs, windows):
        attended = attend(chain, lay, qt, bt, num, top, den, *pair)
        span = (lay.first * width, (lay.first + lay.heads) * width)
        terms.append((attended, 0, *span))
        terms += [(swap(attended, "head", k), k, *span) for k in range(1, sides)]
    late = len(terms) - (sides - 1)
    base = mix(chain, terms[:late], weights, None, F32)
    return mix(chain, terms[late:], weights, base, BF16)


def solution(mesh):
    return jax.shard_map(
        on_device,
        mesh=mesh,
        in_specs=(
            P("ctx", "head", None),
            P("ctx", "head", None),
            P("ctx", "head"),
            P("head", None, None),
            P("head", None),
        ),
        out_specs=P("ctx", "head"),
        check_vma=False,
    )
```
